32 devices in a mesh: pts: 8 (over y, x, core), wid: 4 (over z).
Axes of the slice: x: 2, y: 2, z: 4, core: 2. Of those that a mesh axis runs over, the one named last changes fastest.
Arguments:
- vertex_features: bfloat16 [90112, 512], P('pts'), may hold values from -40 to 40, as said below
- entry_matrix: bfloat16 [512, 512], P(None, 'wid'), may hold values from -2 to 2, as said below
- partition_matrix: bfloat16 [64, 32], replicated, may hold values from -3 to 3, as said below
- sharpness_matrix: float32 [64], replicated, may hold values from -3 to 3, as said below
- summary_qkv_matrix: float32 [3, 64, 64], replicated, may hold values from -3 to 3
- exit_matrix: bfloat16 [512, 512], P('wid'), may hold values from -0.5 to 0.5
- widening_matrix: bfloat16 [512, 512], P('wid'), may hold values from -0.25 to 0.25
- narrowing_matrix: bfloat16 [512, 512], P('wid'), may hold values from -0.25 to 0.25
Outputs:
- result: bfloat16 [90112, 512], P(('pts', 'wid'))
The draws below stay inside these ranges and needn't reach their ends.
Inputs may be any that keep to these rules, and one draw needn't show every extreme that they name: `vertex_features`: features of the points, of order one to ten. `entry_matrix`: weights of the point projection. `partition_matrix`: slice logit weights. `sharpness_matrix`: temperature weights.
All inputs are finite; a program needn't handle non-finite values.
Results may differ from the reference program's by a relative error of at most 0.013.
Values may be sent and summed in bfloat16 or wider, within the bound.
A program may use at most 128 MiB of HBM per device.

```python
import jax
import jax.numpy as jnp
from jax import lax

D = 512
H = 8
DH = 64
G = 32
FF = 512
NPOINTS = 90112


def draw_vertex_features(key, part):
    key_base = jax.random.fold_in(key, 11)
    key_dir = jax.random.fold_in(key, 12)
    key_scale = jax.random.fold_in(key, 13)
    base = jnp.clip(jax.random.normal(key_base, (NPOINTS, D), jnp.float32), -4.0, 4.0)
    spread = jnp.exp(jax.random.uniform(key_scale, (NPOINTS, 1), jnp.float32, 0.0, 1.1))
    direction = jnp.clip(jax.random.normal(key_dir, (1, D), jnp.float32), -4.0, 4.0)
    ramp = 1.0 + 2.0 * jnp.arange(NPOINTS, dtype=jnp.float32)[:, None] / jnp.float32(max(NPOINTS - 1, 1))
    values = base * jnp.minimum(spread, 3.0) + ramp * direction
    values = 0.5 * values
    return jnp.clip(values, -40.0, 40.0).astype(jnp.bfloat16)


def draw_entry_matrix(key, part):
    noise = jnp.clip(jax.random.normal(jax.random.fold_in(key, 21), (D, D), jnp.float32), -6.0, 6.0) / jnp.sqrt(jnp.float32(D))
    return jnp.clip(noise, -2.0, 2.0).astype(jnp.bfloat16)


def draw_partition_matrix(key, part):
    rough = jax.random.normal(jax.random.fold_in(key, 31), (DH, G), jnp.float32)
    values = 0.8 * rough
    return jnp.clip(values, -3.0, 3.0).astype(jnp.bfloat16)


def draw_sharpness_matrix(key, part):
    rough = jax.random.normal(jax.random.fold_in(key, 41), (DH,), jnp.float32)
    values = 0.6 * rough
    return jnp.clip(values, -3.0, 3.0).astype(jnp.float32)


def draw_summary_qkv_matrix(key, part):
    rough = jax.random.normal(jax.random.fold_in(key, 51), (3, DH, DH), jnp.float32)
    values = 0.55 * rough
    return jnp.clip(values, -3.0, 3.0).astype(jnp.float32)


def block_scale(rng, shape, shards, least, top_value):
    level = 1.0
    for axis_at, parts in shards:
        steps = jax.random.uniform(jax.random.fold_in(jax.random.fold_in(rng, 6), axis_at), (parts,), jnp.float32, least / len(shards), top_value / len(shards))
        level = level * jnp.repeat(jnp.exp(steps), shape[axis_at] // parts).reshape((-1,) + (1,) * (len(shape) - 1 - axis_at))
    return level


def normal_values(stream_key, extent, deviation, most, pieces=(), held_as=jnp.bfloat16):
    result = jax.random.normal(stream_key, extent, jnp.float32) * deviation
    if len(pieces) > 0:
        result = block_scale(stream_key, extent, pieces, -0.22, 0.18) * result
    return jnp.clip(result, min=-most, max=most).astype(held_as)


def setup_inputs(seed: int = 0) -> dict:
    arg_keys = jax.random.split(jax.random.key(seed), 9)
    return {
        "vertex_features": draw_vertex_features(jax.random.fold_in(arg_keys[8], 71), 0),
        "entry_matrix": draw_entry_matrix(jax.random.fold_in(arg_keys[8], 71), 0),
        "partition_matrix": draw_partition_matrix(jax.random.fold_in(arg_keys[8], 71), 0),
        "sharpness_matrix": draw_sharpness_matrix(jax.random.fold_in(arg_keys[8], 71), 0),
        "summary_qkv_matrix": draw_summary_qkv_matrix(jax.random.fold_in(arg_keys[8], 71), 0),
        "exit_matrix": normal_values(arg_keys[5], (D, D), (D // 4) ** -0.5, 0.5, ((0, 4),)),
        "widening_matrix": normal_values(arg_keys[6], (D, FF), D ** -0.5, 0.25, ((0, 4),)),
        "narrowing_matrix": normal_values(arg_keys[7], (FF, D), FF ** -0.5, 0.25, ((0, 4),)),
    }


def layer_norm(values):
    centred = values - lax.optimization_barrier(jnp.mean(values, axis=-1, keepdims=True))
    variance = lax.optimization_barrier(jnp.mean(centred * centred, axis=-1, keepdims=True))
    return centred * lax.rsqrt(variance + 1e-05)

def reference(vertex_features, entry_matrix, partition_matrix, sharpness_matrix, summary_qkv_matrix, exit_matrix, widening_matrix, narrowing_matrix):
    features = vertex_features.astype(jnp.float32)
    normed = layer_norm(features).astype(jnp.bfloat16)
    feats = jnp.dot(normed, entry_matrix, preferred_element_type=jnp.float32).astype(jnp.bfloat16)
    attention_cluster = feats.reshape(feats.shape[0], H, DH).astype(jnp.float32)
    partition_sharpness = 0.5 + jax.nn.softplus(jnp.einsum('kgv,v->kg', attention_cluster, sharpness_matrix))
    partition_scores = jnp.einsum('nhd,dg->nhg', attention_cluster, partition_matrix.astype(jnp.float32))
    partition_mapping = jax.nn.softmax(partition_scores / partition_sharpness[:, :, None], axis=-1).astype(jnp.bfloat16)
    weights32 = partition_mapping.astype(jnp.float32)
    numerator = jnp.einsum('nhg,nhd->hgd', weights32, attention_cluster)
    mass = lax.optimization_barrier(jnp.sum(weights32, axis=0))
    token_rows = numerator / (mass[:, :, None] + 1e-05)
    hp = lax.Precision.HIGHEST
    queries = jnp.einsum('hgd,de->hge', token_rows, summary_qkv_matrix[0], precision=hp)
    keys_all = jnp.einsum('hgd,de->hge', token_rows, summary_qkv_matrix[1], precision=hp)
    value_rows_total = jnp.einsum('hgd,de->hge', token_rows, summary_qkv_matrix[2], precision=hp)
    scores = jnp.einsum('hge,hke->hgk', queries, keys_all, precision=hp) / jnp.sqrt(jnp.float32(DH))
    attend = jax.nn.softmax(scores, axis=-1)
    out_tok = jnp.einsum('hgk,hke->hge', attend, value_rows_total, precision=hp).astype(jnp.bfloat16)
    deslice = jnp.einsum('nhg,hgd->nhd', weights32, out_tok.astype(jnp.float32)).astype(jnp.bfloat16)
    deslice = deslice.reshape(feats.shape[0], D)
    midway = features + jnp.dot(deslice, exit_matrix, preferred_element_type=jnp.float32)
    normed2 = layer_norm(midway).astype(jnp.bfloat16)
    hidden = jax.nn.gelu(jnp.dot(normed2, widening_matrix, preferred_element_type=jnp.float32)).astype(jnp.bfloat16)
    return (midway + jnp.dot(hidden, narrowing_matrix, preferred_element_type=jnp.float32)).astype(jnp.bfloat16)
```

```python
import functools
import math

import jax
import jax.numpy as jnp
from jax import lax
from jax.experimental import pallas as pl
from jax.experimental.pallas import tpu as pltpu
from jax.sharding import PartitionSpec as P

MESH = pl.DeviceIdType.MESH
F32 = jnp.float32
BF16 = jnp.bfloat16
HIGH = lax.Precision.HIGHEST
LOG2E = math.log2(math.e)
BOTH = (((1,), (1,)), ((), ()))


def layer_norm(values):
    centred = values - jnp.mean(values, axis=-1, keepdims=True)
    variance = jnp.mean(centred * centred, axis=-1, keepdims=True)
    return centred * lax.rsqrt(variance + 1e-05)


def pick_tile(rows, choices):
    for choice in choices:
        if rows % choice == 0:
            return choice
    return rows


def fold_rows(values, held, combine):
    shift = 4
    while shift >= held:
        values = combine(values, pltpu.roll(values, shift, 0))
        shift //= 2
    return values


def slice_softmax(logits, held, slices):
    wide = held * slices
    raw = logits[wide:wide + 8] + logits[wide + 8:wide + 16]
    soft = jnp.maximum(raw, 0.0) + jnp.log1p(jnp.exp(-jnp.abs(raw)))
    inverse = LOG2E / (0.5 + soft)
    score = logits[:wide].reshape(wide // 8, 8, logits.shape[1]) * inverse[None]
    top = fold_rows(jnp.max(score, axis=0), held, jnp.maximum)
    power = jnp.exp2(score - top[None])
    total = fold_rows(jnp.sum(power, axis=0), held, jnp.add)
    return (power * (1.0 / total)[None]).reshape(wide, logits.shape[1]).astype(BF16)


def fill_logit_mat(mat, part_t, sharp, held, slices, head):
    wide = held * slices
    sharp_hi = sharp.astype(BF16).astype(F32)
    sharp_lo = sharp - sharp_hi
    shape = (wide, head)
    row = lax.broadcasted_iota(jnp.int32, (wide, slices), 0) // held
    col = lax.broadcasted_iota(jnp.int32, (wide, slices), 1)
    pick = jnp.where(row == col, 1.0, 0.0).astype(BF16)
    spread = jnp.dot(pick, part_t, preferred_element_type=F32)
    which = lax.broadcasted_iota(jnp.int32, shape, 0) % held
    small = lax.broadcasted_iota(jnp.int32, (8, head), 0) % held
    for h in range(held):
        lanes = slice(h * head, (h + 1) * head)
        mat[:wide, lanes] = jnp.where(which == h, spread, 0.0)
        mat[wide:wide + 8, lanes] = jnp.where(small == h, sharp_hi, 0.0)
        mat[wide + 8:wide + 16, lanes] = jnp.where(small == h, sharp_lo, 0.0)


def gather_kernel(
    sizes, x_ref, ent_ref, part_hbm, sharp_hbm, qkv_hbm, ex_ref, up_ref, dn_ref,
    w_ref, mix_ref, xo_ref, upg_ref, dng_ref,
    x_all, rows_buf, ent_buf, ext_buf, entt_buf, exg_ref, local_mat, all_mat, num_buf, mass_buf,
    piece_out, piece_in, qkv_ref, big_qkv, tok_buf, part_ref, sharp_ref,
    x_sem, own_sem, zs_sem, zr_sem, fs_sem, fr_sem, cs_sem, cr_sem,
    a_send, a_recv, t_send, t_recv,
):
    pts, wid, share, step, tile, head, slices, heads = sizes
    p, w = lax.axis_index("pts"), lax.axis_index("wid")
    total_rows, model = x_all.shape
    rows = rows_buf.shape[0]
    steps = total_rows // step
    tiles = rows // tile
    chips = share // 2
    group, core = p // share, p % 2
    chip = (p % share) // 2
    member = core * chips + chip
    mine_heads = heads // wid
    local_lanes = mine_heads * head
    local_wide = mine_heads * slices
    held = all_mat.shape[1] // head
    wide = held * slices
    groups = heads // held
    chunk = ex_ref.shape[0]

    def x_copy(t):
        at = pl.ds(pl.multiple_of(t * step, step), step)
        return pltpu.make_async_copy(x_ref.at[at], x_all.at[at], x_sem.at[t])

    small_copies = [
        pltpu.make_async_copy(ent_ref, ent_buf.at[w], own_sem.at[0]),
        pltpu.make_async_copy(part_hbm, part_ref, own_sem.at[1]),
        pltpu.make_async_copy(sharp_hbm, sharp_ref, own_sem.at[2]),
        pltpu.make_async_copy(qkv_hbm, qkv_ref, own_sem.at[3]),
    ]
    for copy in small_copies[:3]:
        copy.start()
    x_copy(0).start()
    own_copies = []
    for m in range(1, 4):
        full = (exg_ref, upg_ref, dng_ref)[m - 1]
        own_copies.append(pltpu.make_async_copy(
            (ex_ref, up_ref, dn_ref)[m - 1],
            full.at[pl.ds(pl.multiple_of(w * chunk, chunk), chunk)], own_sem.at[m + 3],
        ))
    for copy in own_copies:
        copy.start()
    for t in range(1, steps):
        x_copy(t).start()
    small_copies[3].start()
    own_rows = pltpu.make_async_copy(
        x_ref.at[pl.ds(pl.multiple_of(w * rows, rows), rows)], xo_ref, own_sem.at[7]
    )
    own_rows.start()

    barrier = pltpu.get_barrier_semaphore()
    for d in range(1, wid):
        pl.semaphore_signal(
            barrier, inc=1, device_id=(p, lax.rem(w + d, wid)), device_id_type=MESH
        )
    for d in range(1, pts):
        pl.semaphore_signal(
            barrier, inc=1, device_id=(lax.rem(p + d, pts), w), device_id_type=MESH
        )

    ent_part = ent_ref.shape[0] // share
    out_part = chunk // share

    def spot(m, owner, part, parts=1):
        if m == 0:
            count = ent_part * parts
            return ent_buf.at[owner, pl.ds(pl.multiple_of(part * count, count), count)]
        count = out_part * parts
        full = (exg_ref, upg_ref, dng_ref)[m - 1]
        return full.at[pl.ds(pl.multiple_of(owner * chunk + part * count, count), count)]

    def across(m, d):
        return pltpu.make_async_remote_copy(
            src_ref=spot(m, w, member), dst_ref=spot(m, w, member),
            send_sem=zs_sem.at[m, d - 1], recv_sem=zr_sem.at[m, d - 1],
            device_id=(p, lax.rem(w + d, wid)), device_id_type=MESH,
        )

    def forward(m, d, e):
        owner = lax.rem(w - d + wid, wid)
        to = group * share + 2 * lax.rem(chip + e, chips) + core
        return pltpu.make_async_remote_copy(
            src_ref=spot(m, owner, member), dst_ref=spot(m, owner, member),
            send_sem=fs_sem.at[m, d - 1, e - 1], recv_sem=fr_sem.at[m, d - 1, e - 1],
            device_id=(to, w), device_id_type=MESH,
        )

    def swap(m, d):
        owner = lax.rem(w - d + wid, wid)
        half = spot(m, owner, core, chips)
        return pltpu.make_async_remote_copy(
            src_ref=half, dst_ref=half,
            send_sem=cs_sem.at[m, d - 1], recv_sem=cr_sem.at[m, d - 1],
            device_id=(p + 1 - 2 * core, w), device_id_type=MESH,
        )

    def cross_all():
        for m in range(4):
            for d in range(1, wid):
                across(m, d).start()

    def pass_on(m):
        for d in range(1, wid):
            across(m, d).wait_recv()
            for e in range(1, chips):
                forward(m, d, e).start()

    def trade(m):
        for d in range(1, wid):
            for e in range(1, chips):
                forward(m, d, e).wait_recv()
            swap(m, d).start()

    def traded(m):
        for d in range(1, wid):
            swap(m, d).wait_recv()

    ext_buf[...] = jnp.zeros_like(ext_buf)
    ext_buf[:, 128:] = jnp.ones((model, 128), BF16)
    piece_out[...] = jnp.zeros_like(piece_out)
    num_buf[...] = jnp.zeros_like(num_buf)
    mass_buf[...] = jnp.zeros_like(mass_buf)
    local_mat[...] = jnp.zeros_like(local_mat)
    all_mat[...] = jnp.zeros_like(all_mat)
    big_qkv[...] = jnp.zeros_like(big_qkv)
    tok_buf[...] = jnp.zeros_like(tok_buf)
    for copy in small_copies[:3]:
        copy.wait()
    part_t, sharp = part_ref[...], sharp_ref[...]
    fill_logit_mat(local_mat, part_t, sharp, mine_heads, slices, head)
    fill_logit_mat(all_mat, part_t, sharp, held, slices, head)
    ext_buf[:, :local_lanes] = ent_buf[w]
    column_sum = jnp.sum(ext_buf[:, :128].astype(F32), axis=0, keepdims=True)
    local_lhs = local_mat[...].astype(BF16)

    def numerator_step(t, carry):
        @pl.when(t == 1)
        def _():
            pl.semaphore_wait(barrier, wid - 1 + pts - 1)
            for copy in own_copies:
                copy.wait()
            cross_all()

        @pl.when(t == steps - 2)
        def _():
            pass_on(0)

        x_copy(t).wait()
        at = pl.ds(pl.multiple_of(t * step, step), step)
        narrow = x_all[at, :]
        raw = jnp.dot(narrow, ext_buf[...], preferred_element_type=F32)
        mean = raw[:, 128:] * (1.0 / model)
        wider = narrow.astype(F32)
        centred = wider - jnp.concatenate([mean] * (model // 128), axis=1)
        variance = jnp.sum(centred * centred, axis=1, keepdims=True) * (1.0 / model)
        feats = ((raw[:, :128] - mean * column_sum) * lax.rsqrt(variance + 1e-05)).astype(BF16)
        logits = lax.dot_general(local_lhs, feats, BOTH, preferred_element_type=F32)
        block = slice_softmax(logits, mine_heads, slices)
        num_buf[...] += jnp.dot(block, feats, preferred_element_type=F32)
        rounded = block.astype(F32)
        mass = rounded[:, :128]
        for c in range(1, step // 128):
            mass = mass + rounded[:, c * 128:(c + 1) * 128]
        mass_buf[...] += mass
        return carry

    lax.fori_loop(0, steps, numerator_step, 0)

    lane = lax.broadcasted_iota(jnp.int32, (slices, 128), 1)
    packed = jnp.zeros((slices, 128), F32)
    for h in range(mine_heads):
        packed = jnp.where(lane // head == h, num_buf[pl.ds(h, slices, stride=mine_heads), :], packed)
    piece_out[:slices, :] = packed
    piece_out[slices:, :local_wide] = lax.dot_general(
        jnp.ones((8, 128), F32), mass_buf[...], BOTH, precision=HIGH, preferred_element_type=F32
    )
    spread = []
    for d in range(1, pts):
        spread.append(pltpu.make_async_remote_copy(
            src_ref=piece_out, dst_ref=piece_in.at[d - 1],
            send_sem=a_send.at[d - 1], recv_sem=a_recv.at[d - 1],
            device_id=(lax.rem(p + d, pts), w), device_id_type=MESH,
        ))
    for copy in spread:
        copy.start()

    for m in range(1, 4):
        pass_on(m)
    small_copies[3].wait()
    for i in range(3):
        for h in range(mine_heads):
            at = slice(h * head, (h + 1) * head)
            big_qkv[i, at, at] = qkv_ref[i]

    own_rows.wait()
    norm_tile = pick_tile(rows, (704, 256, 128))

    def norm_step(t, carry):
        at = pl.ds(pl.multiple_of(t * norm_tile, norm_tile), norm_tile)
        rows_buf[at, :] = layer_norm(xo_ref[at, :].astype(F32)).astype(BF16)
        return carry

    lax.fori_loop(0, rows // norm_tile, norm_step, 0)
    trade(0)

    total = piece_out[...]
    for d in range(1, pts):
        spread[d - 1].wait_recv()
        total = total + piece_in[d - 1]
    row = lax.broadcasted_iota(jnp.int32, (slices, local_wide), 0)
    col = lax.broadcasted_iota(jnp.int32, (slices, local_wide), 1)
    masses = jnp.ones((slices, 128), F32)
    for h in range(mine_heads):
        one = jnp.sum(
            jnp.where(col == row * mine_heads + h, total[slices:slices + 1, :local_wide], 0.0),
            axis=1, keepdims=True,
        )
        masses = jnp.where(lane // head == h, one, masses)
    tokens = total[:slices] / (masses + 1e-05)
    queries, keys_all, value_rows = (
        jnp.dot(tokens, big_qkv[i], precision=HIGH, preferred_element_type=F32) for i in range(3)
    )
    stacked = lambda a: jnp.concatenate(
        [jnp.where(lane // head == h, a, 0.0) for h in range(mine_heads)], axis=0
    )
    scores = lax.dot_general(
        queries, stacked(keys_all), BOTH, precision=HIGH, preferred_element_type=F32
    ) * (1.0 / head ** 0.5)
    owner_head = col // slices
    attend = jnp.zeros_like(scores)
    for h in range(mine_heads):
        part = jnp.where(owner_head == h, scores, -jnp.inf)
        power = jnp.exp(part - jnp.max(part, axis=1, keepdims=True))
        attend = attend + power / jnp.sum(power, axis=1, keepdims=True)
    tok_buf[w] = jnp.dot(
        attend, stacked(value_rows), precision=HIGH, preferred_element_type=F32
    ).astype(BF16)
    ring = []
    for d in range(1, wid):
        ring.append(pltpu.make_async_remote_copy(
            src_ref=tok_buf.at[w], dst_ref=tok_buf.at[w],
            send_sem=t_send.at[d - 1], recv_sem=t_recv.at[d - 1],
            device_id=(p, lax.rem(w + d, wid)), device_id_type=MESH,
        ))
    for copy in ring:
        copy.start()

    traded(0)
    trade(1)
    width = ent_ref.shape[1]
    for owner in range(wid):
        entt_buf[owner * width:(owner + 1) * width, :] = ent_buf[owner].T
    lhs = all_mat[...].astype(BF16)

    def slice_step(t, carry):
        at = pl.ds(pl.multiple_of(t * tile, tile), tile)
        feats = lax.dot_general(
            entt_buf[...], rows_buf[at, :], BOTH, preferred_element_type=F32
        ).astype(BF16)
        for gi in range(groups):
            own = feats[gi * held * head:(gi + 1) * held * head]
            logits = jnp.dot(lhs, own, preferred_element_type=F32)
            w_ref[at, gi * wide:(gi + 1) * wide] = slice_softmax(logits, held, slices).T
        return carry

    lax.fori_loop(0, tiles, slice_step, 0)
    for m in range(2, 4):
        trade(m)
    traded(1)
    for copy in ring:
        copy.wait_recv()

    row = lax.broadcasted_iota(jnp.int32, (wide, slices), 0) // held
    col = lax.broadcasted_iota(jnp.int32, (wide, slices), 1)
    repeat = jnp.where(row == col, 1.0, 0.0).astype(BF16)
    row = lax.broadcasted_iota(jnp.int32, (wide, held * head), 0) % held
    col = lax.broadcasted_iota(jnp.int32, (wide, held * head), 1) // head
    every = jnp.concatenate(
        [tok_buf[z].astype(F32)[:, :local_lanes] for z in range(wid)], axis=1
    ).astype(BF16)
    for gi in range(groups):
        lanes = slice(gi * held * head, (gi + 1) * held * head)
        block = jnp.dot(repeat, every[:, lanes], preferred_element_type=F32)
        block = jnp.where(row == col, block, 0.0).astype(BF16)
        mix_ref[gi * wide:(gi + 1) * wide, :] = jnp.dot(
            block, exg_ref[lanes, :], preferred_element_type=F32
        ).astype(BF16)
    for m in range(2, 4):
        traded(m)
    for m in range(4):
        for d in range(1, wid):
            across(m, d).wait_send()
            swap(m, d).wait_send()
            for e in range(1, chips):
                forward(m, d, e).wait_send()
    for copy in spread + ring:
        copy.wait_send()


def rows_kernel(step, w_ref, mix_ref, x_ref, upg_ref, dng_ref, out_ref, out_buf, out_sem):
    steps = x_ref.shape[0] // step

    def out_copy(t, slot):
        at = pl.ds(pl.multiple_of(t * step, step), step)
        return pltpu.make_async_copy(out_buf.at[slot], out_ref.at[at], out_sem.at[slot])

    def feed_step(t, carry):
        slot = lax.rem(t, 2)
        at = pl.ds(pl.multiple_of(t * step, step), step)
        midway = x_ref[at, :].astype(F32) + jnp.dot(
            w_ref[at, :], mix_ref[...], preferred_element_type=F32
        )
        normed = layer_norm(midway).astype(BF16)
        hidden = jax.nn.gelu(
            jnp.dot(normed, upg_ref[...], preferred_element_type=F32)
        ).astype(BF16)
        result = (
            midway + jnp.dot(hidden, dng_ref[...], preferred_element_type=F32)
        ).astype(BF16)

        @pl.when(t >= 2)
        def _():
            out_copy(t - 2, slot).wait()

        out_buf[slot] = result
        out_copy(t, slot).start()
        return carry

    lax.fori_loop(0, steps, feed_step, 0)
    for t in range(max(steps - 2, 0), steps):
        out_copy(t, t % 2).wait()


def local(x, entry, partition, sharpness, qkv, exit_m, widening, narrowing):
    pts, wid = lax.axis_size("pts"), lax.axis_size("wid")
    width = x.shape[1]
    head, slices = partition.shape
    heads = entry.shape[1] * wid // head
    mine = heads // wid
    rows = x.shape[0] // wid
    chunk = exit_m.shape[0]
    cells = heads * slices
    step = pick_tile(x.shape[0], (1408, 1024, 512, 256, 128))
    tile = pick_tile(rows, (1408, 256, 128))
    held = 256 // head
    share = 2
    for choice in (8, 4):
        if pts % choice == 0 and chunk % (16 * choice) == 0:
            share = choice
            break
    sizes = (pts, wid, share, step, tile, head, slices, heads)
    vmem = pl.BlockSpec(memory_space=pltpu.VMEM)
    hbm = pl.BlockSpec(memory_space=pltpu.HBM)
    dma = pltpu.SemaphoreType.DMA
    full = pltpu.VMEM((chunk * wid, width), BF16)
    hops = max(share // 2 - 1, 1)
    x = pltpu.with_memory_space_constraint(x, pltpu.HBM)
    weights, mix, own, upg, dng = pl.pallas_call(
        functools.partial(gather_kernel, sizes),
        name="slices_and_gather",
        out_shape=(
            pltpu.VMEM((rows, cells), BF16),
            pltpu.VMEM((cells, width), BF16),
            pltpu.VMEM((rows, width), BF16),
            full, full,
        ),
        in_specs=[hbm] * 8,
        out_specs=(vmem,) * 5,
        scratch_shapes=[
            pltpu.VMEM(x.shape, BF16),
            pltpu.VMEM((rows, width), BF16),
            pltpu.VMEM((wid,) + entry.shape, BF16),
            pltpu.VMEM((width, 256), BF16),
            pltpu.VMEM((entry.shape[1] * wid, entry.shape[0]), BF16),
            pltpu.VMEM((chunk * wid, width), BF16),
            pltpu.VMEM((mine * slices + 16, 128), F32),
            pltpu.VMEM((held * slices + 16, held * head), F32),
            pltpu.VMEM((mine * slices, 128), F32),
            pltpu.VMEM((mine * slices, 128), F32),
            pltpu.VMEM((slices + 8, 128), F32),
            pltpu.VMEM((pts - 1, slices + 8, 128), F32),
            pltpu.VMEM(qkv.shape, F32),
            pltpu.VMEM((3, 128, 128), F32),
            pltpu.VMEM((wid, slices, 128), BF16),
            pltpu.VMEM((slices, head), BF16),
            pltpu.VMEM((1, head), F32),
            dma((x.shape[0] // step,)), dma((8,)),
            dma((4, wid - 1)), dma((4, wid - 1)),
            dma((4, wid - 1, hops)), dma((4, wid - 1, hops)),
            dma((4, wid - 1)), dma((4, wid - 1)),
            dma((pts - 1,)), dma((pts - 1,)),
            dma((wid - 1,)), dma((wid - 1,)),
        ],
        compiler_params=pltpu.CompilerParams(
            collective_id=0, has_side_effects=True, vmem_limit_bytes=44 * 1024 * 1024
        ),
    )(x, entry, partition.T, sharpness.reshape(1, head), qkv, exit_m, widening, narrowing)

    step = pick_tile(rows, (704, 256, 128))
    return pl.pallas_call(
        functools.partial(rows_kernel, step),
        name="mix_and_feed",
        out_shape=jax.ShapeDtypeStruct((rows, width), BF16),
        in_specs=[vmem] * 5,
        out_specs=pl.BlockSpec(memory_space=pl.ANY),
        scratch_shapes=[pltpu.VMEM((2, step, width), BF16), dma((2,))],
        compiler_params=pltpu.CompilerParams(vmem_limit_bytes=40 * 1024 * 1024),
    )(weights, mix, own, upg, dng)


def solution(mesh):
    placed = (
        P("pts", None),
        P(None, "wid"),
        P(),
        P(),
        P(),
        P("wid", None),
        P("wid", None),
        P("wid", None),
    )
    return jax.shard_map(
        local, mesh=mesh, in_specs=placed, out_specs=P(("pts", "wid"), None), check_vma=False
    )
```

```python
import functools
import math

import jax
import jax.numpy as jnp
from jax import lax
from jax.experimental import pallas as pl
from jax.experimental.pallas import tpu as pltpu
from jax.sharding import PartitionSpec as P

MESH = pl.DeviceIdType.MESH
F32 = jnp.float32
BF16 = jnp.bfloat16
HIGH = lax.Precision.HIGHEST
LOG2E = math.log2(math.e)
BOTH = (((1,), (1,)), ((), ()))
GELU_A = math.sqrt(2.0 / math.pi)
GELU_B = 0.044715 * math.sqrt(2.0 / math.pi)


def layer_norm(values):
    centred = values - jnp.mean(values, axis=-1, keepdims=True)
    variance = jnp.mean(centred * centred, axis=-1, keepdims=True)
    return centred * lax.rsqrt(variance + 1e-05)


def pick_tile(rows, choices):
    for choice in choices:
        if rows % choice == 0:
            return choice
    return rows


def fold_rows(values, held, combine):
    shift = 4
    while shift >= held:
        values = combine(values, pltpu.roll(values, shift, 0))
        shift //= 2
    return values


def slice_softmax(logits, held, slices):
    wide = held * slices
    raw = logits[wide:wide + 8] + logits[wide + 8:wide + 16]
    soft = jnp.maximum(raw, 0.0) + jnp.log1p(jnp.exp(-jnp.abs(raw)))
    inverse = LOG2E / (0.5 + soft)
    score = logits[:wide].reshape(wide // 8, 8, logits.shape[1]) * inverse[None]
    top = fold_rows(jnp.max(score, axis=0), held, jnp.maximum)
    power = jnp.exp2(score - top[None])
    total = fold_rows(jnp.sum(power, axis=0), held, jnp.add)
    return (power * (1.0 / total)[None]).reshape(wide, logits.shape[1]).astype(BF16)


def fill_logit_mat(mat, part_t, sharp, held, slices, head):
    wide = held * slices
    sharp_hi = sharp.astype(BF16).astype(F32)
    sharp_lo = sharp - sharp_hi
    shape = (wide, head)
    row = lax.broadcasted_iota(jnp.int32, (wide, slices), 0) // held
    col = lax.broadcasted_iota(jnp.int32, (wide, slices), 1)
    pick = jnp.where(row == col, 1.0, 0.0).astype(BF16)
    spread = jnp.dot(pick, part_t, preferred_element_type=F32)
    which = lax.broadcasted_iota(jnp.int32, shape, 0) % held
    small = lax.broadcasted_iota(jnp.int32, (8, head), 0) % held
    for h in range(held):
        lanes = slice(h * head, (h + 1) * head)
        mat[:wide, lanes] = jnp.where(which == h, spread, 0.0)
        mat[wide:wide + 8, lanes] = jnp.where(small == h, sharp_hi, 0.0)
        mat[wide + 8:wide + 16, lanes] = jnp.where(small == h, sharp_lo, 0.0)


def gather_kernel(
    sizes, x_ref, ent_ref, part_hbm, sharp_hbm, qkv_hbm, ex_ref, up_ref, dn_ref,
    w_ref, mix_ref, xo_ref, upg_ref, dng_ref,
    x_all, rows_buf, ent_buf, ext_buf, feats_buf, raw_buf, entt_buf, exg_ref, local_mat, all_mat, num_buf, mass_buf,
    piece_out, piece_in, qkv_ref, big_qkv, tok_buf, part_ref, sharp_ref,
    x_sem, own_sem, zs_sem, zr_sem, fs_sem, fr_sem, cs_sem, cr_sem,
    a_send, a_recv, t_send, t_recv,
):
    pts, wid, share, step, tile, head, slices, heads = sizes
    p, w = lax.axis_index("pts"), lax.axis_index("wid")
    total_rows, model = x_all.shape
    rows = rows_buf.shape[0]
    steps = total_rows // step
    tiles = rows // tile
    chips = share // 2
    group, core = p // share, p % 2
    chip = (p % share) // 2
    member = core * chips + chip
    mine_heads = heads // wid
    local_lanes = mine_heads * head
    local_wide = mine_heads * slices
    held = all_mat.shape[1] // head
    wide = held * slices
    groups = heads // held
    chunk = ex_ref.shape[0]

    def x_copy(t):
        at = pl.ds(pl.multiple_of(t * step, step), step)
        return pltpu.make_async_copy(x_ref.at[at], x_all.at[at], x_sem.at[t])

    small_copies = [
        pltpu.make_async_copy(ent_ref, ent_buf.at[w], own_sem.at[0]),
        pltpu.make_async_copy(part_hbm, part_ref, own_sem.at[1]),
        pltpu.make_async_copy(sharp_hbm, sharp_ref, own_sem.at[2]),
        pltpu.make_async_copy(qkv_hbm, qkv_ref, own_sem.at[3]),
    ]
    for copy in small_copies[:1]:
        copy.start()
    x_copy(0).start()
    for copy in small_copies[1:3]:
        copy.start()
    own_copies = []
    for m in range(1, 4):
        full = (exg_ref, upg_ref, dng_ref)[m - 1]
        own_copies.append(pltpu.make_async_copy(
            (ex_ref, up_ref, dn_ref)[m - 1],
            full.at[pl.ds(pl.multiple_of(w * chunk, chunk), chunk)], own_sem.at[m + 3],
        ))
    own_rows = pltpu.make_async_copy(
        x_ref.at[pl.ds(pl.multiple_of(w * rows, rows), rows)], xo_ref, own_sem.at[7]
    )

    barrier = pltpu.get_barrier_semaphore()
    for d in range(1, wid):
        pl.semaphore_signal(
            barrier, inc=1, device_id=(p, lax.rem(w + d, wid)), device_id_type=MESH
        )
    for d in range(1, pts):
        pl.semaphore_signal(
            barrier, inc=1, device_id=(lax.rem(p + d, pts), w), device_id_type=MESH
        )

    ent_part = ent_ref.shape[0] // share
    out_part = chunk // share

    def spot(m, owner, part, parts=1):
        if m == 0:
            count = ent_part * parts
            return ent_buf.at[owner, pl.ds(pl.multiple_of(part * count, count), count)]
        count = out_part * parts
        full = (exg_ref, upg_ref, dng_ref)[m - 1]
        return full.at[pl.ds(pl.multiple_of(owner * chunk + part * count, count), count)]

    def across(m, d):
        return pltpu.make_async_remote_copy(
            src_ref=spot(m, w, member), dst_ref=spot(m, w, member),
            send_sem=zs_sem.at[m, d - 1], recv_sem=zr_sem.at[m, d - 1],
            device_id=(p, lax.rem(w + d, wid)), device_id_type=MESH,
        )

    def forward(m, d, e):
        owner = lax.rem(w - d + wid, wid)
        to = group * share + 2 * lax.rem(chip + e, chips) + core
        return pltpu.make_async_remote_copy(
            src_ref=spot(m, owner, member), dst_ref=spot(m, owner, member),
            send_sem=fs_sem.at[m, d - 1, e - 1], recv_sem=fr_sem.at[m, d - 1, e - 1],
            device_id=(to, w), device_id_type=MESH,
        )

    def swap(m, d):
        owner = lax.rem(w - d + wid, wid)
        half = spot(m, owner, core, chips)
        return pltpu.make_async_remote_copy(
            src_ref=half, dst_ref=half,
            send_sem=cs_sem.at[m, d - 1], recv_sem=cr_sem.at[m, d - 1],
            device_id=(p + 1 - 2 * core, w), device_id_type=MESH,
        )

    def cross_all():
        for m in range(4):
            for d in range(1, wid):
                across(m, d).start()

    def pass_on(m):
        for d in range(1, wid):
            across(m, d).wait_recv()
            for e in range(1, chips):
                forward(m, d, e).start()

    def trade(m):
        for d in range(1, wid):
            for e in range(1, chips):
                forward(m, d, e).wait_recv()
            swap(m, d).start()

    def traded(m):
        for d in range(1, wid):
            swap(m, d).wait_recv()

    with jax.named_scope("setup"):
        ext_buf[:, :128] = jnp.zeros((model, 128), BF16)
        ext_buf[:, 128:] = jnp.full((model, 128), 1.0 / model, BF16)
        piece_out[...] = jnp.zeros_like(piece_out)
        num_buf[...] = jnp.zeros_like(num_buf)
        mass_buf[...] = jnp.zeros_like(mass_buf)
        local_mat[...] = jnp.zeros_like(local_mat)
        small_copies[0].wait()
        ext_buf[:, :local_lanes] = ent_buf[w]
        column_sum = jnp.sum(ext_buf[:, :128].astype(F32), axis=0, keepdims=True)
        x_copy(1).start()
        for copy in own_copies:
            copy.start()
        for t in range(2, min(4, steps)):
            x_copy(t).start()

    def tile_at(t):
        return pl.ds(pl.multiple_of(t * step, step), step)

    def project(t):
        return jnp.dot(x_all[tile_at(t), :], ext_buf[...], preferred_element_type=F32)

    def normalise(t, raw):
        narrow = x_all[tile_at(t), :]
        mean = raw[:, 128:]
        near = mean.astype(BF16)
        shift = mean - near.astype(F32)
        centred = narrow - jnp.concatenate([near] * (model // 128), axis=1)
        square = centred * centred
        while square.shape[1] > 128:
            half = square.shape[1] // 2
            square = square[:, :half] + square[:, half:]
        second = jnp.sum(square.astype(F32), axis=1, keepdims=True) * (1.0 / model)
        scale = lax.rsqrt(second - shift * shift + 1e-05)
        return ((raw[:, :128] - mean * column_sum) * scale).astype(BF16)

    def logits_of(feats):
        return lax.dot_general(local_mat[...].astype(BF16), feats, BOTH, preferred_element_type=F32)

    def collect(block, feats):
        num_buf[...] += jnp.dot(block, feats, preferred_element_type=F32)
        rounded = block.astype(F32)
        mass = rounded[:, :128]
        for c in range(1, block.shape[1] // 128):
            mass = mass + rounded[:, c * 128:(c + 1) * 128]
        mass_buf[...] += mass

    middle = (step // 128 + 1) // 2 * 128
    cuts = [slice(0, middle)] + ([slice(middle, step)] if middle < step else [])

    def ready(t):
        with jax.named_scope("xwait"):
            x_copy(t).wait()

    def fetch(t):
        if isinstance(t, int):
            if t < steps:
                x_copy(t).start()
        else:
            @pl.when(t < steps)
            def _():
                x_copy(t).start()

    def stage(t, slot, ahead):
        other = 1 - slot
        if ahead > 0:
            feats_buf[other] = normalise(t + 1, raw_buf[other])
        parts = [feats_buf[slot, c] for c in cuts]
        logits = [logits_of(part) for part in parts]
        if ahead > 1:
            raw_buf[slot] = project(t + 2)
        for one, part in zip(logits, parts):
            collect(slice_softmax(one, mine_heads, slices), part)

    pairs = (steps - 2) // 2

    def pair_step(i, carry):
        @pl.when(i == 0)
        def _():
            with jax.named_scope("barrier"):
                pl.semaphore_wait(barrier, wid - 1 + pts - 1)
                for copy in own_copies:
                    copy.wait()
                cross_all()

        @pl.when(i == pairs - 1)
        def _():
            with jax.named_scope("pass0"):
                pass_on(0)

        ready(2 * i + 2)
        ready(2 * i + 3)
        fetch(2 * i + 4)
        fetch(2 * i + 5)
        stage(2 * i, 0, 2)
        stage(2 * i + 1, 1, 2)
        return carry

    with jax.named_scope("numer"):
        x_copy(0).wait()
        raw_buf[0] = project(0)
        for copy in small_copies[1:3]:
            copy.wait()
        fill_logit_mat(local_mat, part_ref[...], sharp_ref[...], mine_heads, slices, head)
        x_copy(1).wait()
        feats_buf[0] = normalise(0, raw_buf[0])
        raw_buf[1] = project(1)
        lax.fori_loop(0, pairs, pair_step, 0)
        own_rows.start()
        small_copies[3].start()
        with jax.named_scope("pass1"):
            pass_on(1)
        for t in range(2 * pairs + 2, steps):
            ready(t)
        for t in range(2 * pairs, steps):
            stage(t, t % 2, min(2, steps - 1 - t))
    with jax.named_scope("pack"):
        lane = lax.broadcasted_iota(jnp.int32, (slices, 128), 1)
        packed = jnp.zeros((slices, 128), F32)
        for h in range(mine_heads):
            packed = jnp.where(lane // head == h, num_buf[pl.ds(h, slices, stride=mine_heads), :], packed)
        piece_out[:slices, :] = packed
        piece_out[slices:, :local_wide] = lax.dot_general(
            jnp.ones((8, 128), F32), mass_buf[...], BOTH, precision=HIGH, preferred_element_type=F32
        )
        spread = []
        for d in range(1, pts):
            spread.append(pltpu.make_async_remote_copy(
                src_ref=piece_out, dst_ref=piece_in.at[d - 1],
                send_sem=a_send.at[d - 1], recv_sem=a_recv.at[d - 1],
                device_id=(lax.rem(p + d, pts), w), device_id_type=MESH,
            ))
        for copy in spread:
            copy.start()
    with jax.named_scope("pass23"):
        trade(0)
        for m in range(2, 4):
            pass_on(m)
    with jax.named_scope("fill"):
        all_mat[...] = jnp.zeros_like(all_mat)
        big_qkv[...] = jnp.zeros_like(big_qkv)
        fill_logit_mat(all_mat, part_ref[...], sharp_ref[...], held, slices, head)
        small_copies[3].wait()
        for i in range(3):
            for h in range(mine_heads):
                at = slice(h * head, (h + 1) * head)
                big_qkv[i, at, at] = qkv_ref[i]
    own_rows.wait()
    norm_tile = pick_tile(rows, (704, 256, 128))

    def norm_step(t, carry):
        at = pl.ds(pl.multiple_of(t * norm_tile, norm_tile), norm_tile)
        rows_buf[at, :] = layer_norm(xo_ref[at, :].astype(F32)).astype(BF16)
        return carry

    with jax.named_scope("norm"):
        lax.fori_loop(0, rows // norm_tile, norm_step, 0)
    with jax.named_scope("traded0"):
        traded(0)
        trade(1)
    with jax.named_scope("entt"):
        width = ent_ref.shape[1]
        for owner in range(wid):
            entt_buf[owner * width:(owner + 1) * width, :] = ent_buf[owner].T

    def slice_step(t, carry):
        at = pl.ds(pl.multiple_of(t * tile, tile), tile)
        feats = lax.dot_general(
            entt_buf[...], rows_buf[at, :], BOTH, preferred_element_type=F32
        ).astype(BF16)
        lhs = all_mat[...].astype(BF16)
        for gi in range(groups):
            own = feats[gi * held * head:(gi + 1) * held * head]
            logits = jnp.dot(lhs, own, preferred_element_type=F32)
            w_ref[at, gi * wide:(gi + 1) * wide] = slice_softmax(logits, held, slices).T
        return carry

    with jax.named_scope("slice"):
        lax.fori_loop(0, tiles // 2, slice_step, 0)
    with jax.named_scope("sumwait"):
        total = piece_out[...]
        for d in range(1, pts):
            spread[d - 1].wait_recv()
            total = total + piece_in[d - 1]
    with jax.named_scope("token"):
        row = lax.broadcasted_iota(jnp.int32, (slices, local_wide), 0)
        col = lax.broadcasted_iota(jnp.int32, (slices, local_wide), 1)
        masses = jnp.ones((slices, 128), F32)
        for h in range(mine_heads):
            one = jnp.sum(
                jnp.where(col == row * mine_heads + h, total[slices:slices + 1, :local_wide], 0.0),
                axis=1, keepdims=True,
            )
            masses = jnp.where(lane // head == h, one, masses)
        tokens = total[:slices] / (masses + 1e-05)
        queries, keys_all, value_rows = (
            jnp.dot(tokens, big_qkv[i], precision=HIGH, preferred_element_type=F32) for i in range(3)
        )
        stacked = lambda a: jnp.concatenate(
            [jnp.where(lane // head == h, a, 0.0) for h in range(mine_heads)], axis=0
        )
        scores = lax.dot_general(
            queries, stacked(keys_all), BOTH, precision=HIGH, preferred_element_type=F32
        ) * (1.0 / head ** 0.5)
        owner_head = col // slices
        attend = jnp.zeros_like(scores)
        for h in range(mine_heads):
            part = jnp.where(owner_head == h, scores, -jnp.inf)
            power = jnp.exp(part - jnp.max(part, axis=1, keepdims=True))
            attend = attend + power / jnp.sum(power, axis=1, keepdims=True)
        tok_buf[w] = jnp.dot(
            attend, stacked(value_rows), precision=HIGH, preferred_element_type=F32
        ).astype(BF16)
        ring = []
        for d in range(1, wid):
            ring.append(pltpu.make_async_remote_copy(
                src_ref=tok_buf.at[w], dst_ref=tok_buf.at[w],
                send_sem=t_send.at[d - 1], recv_sem=t_recv.at[d - 1],
                device_id=(p, lax.rem(w + d, wid)), device_id_type=MESH,
            ))
        for copy in ring:
            copy.start()
    with jax.named_scope("slice"):
        lax.fori_loop(tiles // 2, tiles, slice_step, 0)
    with jax.named_scope("ringwait"):
        for m in range(2, 4):
            trade(m)
        traded(1)
        for copy in ring:
            copy.wait_recv()
    with jax.named_scope("mix"):
        row = lax.broadcasted_iota(jnp.int32, (wide, slices), 0) // held
        col = lax.broadcasted_iota(jnp.int32, (wide, slices), 1)
        repeat = jnp.where(row == col, 1.0, 0.0).astype(BF16)
        row = lax.broadcasted_iota(jnp.int32, (wide, held * head), 0) % held
        col = lax.broadcasted_iota(jnp.int32, (wide, held * head), 1) // head
        every = jnp.concatenate(
            [tok_buf[z].astype(F32)[:, :local_lanes] for z in range(wid)], axis=1
        ).astype(BF16)
        for gi in range(groups):
            lanes = slice(gi * held * head, (gi + 1) * held * head)
            block = jnp.dot(repeat, every[:, lanes], preferred_element_type=F32)
            block = jnp.where(row == col, block, 0.0).astype(BF16)
            mix_ref[gi * wide:(gi + 1) * wide, :] = jnp.dot(
                block, exg_ref[lanes, :], preferred_element_type=F32
            ).astype(BF16)
    with jax.named_scope("drain"):
        for m in range(2, 4):
            traded(m)
        for m in range(4):
            for d in range(1, wid):
                across(m, d).wait_send()
                swap(m, d).wait_send()
                for e in range(1, chips):
                    forward(m, d, e).wait_send()
        for copy in spread + ring:
            copy.wait_send()


def rows_kernel(
    step, w_ref, mix_ref, x_ref, upg_ref, dng_ref, out_ref,
    mid_buf, normed_buf, out_buf, out_sem,
):
    steps = x_ref.shape[0] // step
    model = x_ref.shape[1]

    def tile_at(t):
        return pl.ds(pl.multiple_of(t * step, step), step)

    def out_copy(t):
        return pltpu.make_async_copy(out_buf.at[t], out_ref.at[tile_at(t)], out_sem.at[t])

    def mix(t, slot):
        at = tile_at(t)
        midway = x_ref[at, :].astype(F32) + jnp.dot(
            w_ref[at, :], mix_ref[...], preferred_element_type=F32
        )
        mid_buf[slot] = midway
        centred = (midway - jnp.mean(midway, axis=1, keepdims=True)).astype(BF16)
        square = centred * centred
        while square.shape[1] > 128:
            half = square.shape[1] // 2
            square = square[:, :half] + square[:, half:]
        variance = jnp.sum(square.astype(F32), axis=1, keepdims=True) * (1.0 / model)
        scale = lax.rsqrt(variance + 1e-05).astype(BF16)
        normed_buf[slot] = centred * scale

    def feed(t, slot):
        before = jnp.dot(
            normed_buf[slot], upg_ref[...], preferred_element_type=F32
        ).astype(BF16)
        inner = before * (GELU_A + GELU_B * (before * before))
        half = 0.5 * before
        hidden = half + half * jnp.tanh(inner)
        out_buf[t] = (
            mid_buf[slot] + jnp.dot(hidden, dng_ref[...], preferred_element_type=F32)
        ).astype(BF16)

    with jax.named_scope("first"):
        mix(0, 0)
    for t in range(steps):
        with jax.named_scope("tail"):
            slot = t % 2
            if t + 1 < steps:
                mix(t + 1, 1 - slot)
            feed(t, slot)
            out_copy(t).start()
    with jax.named_scope("outwait"):
        for t in range(steps):
            out_copy(t).wait()


def local(x, entry, partition, sharpness, qkv, exit_m, widening, narrowing):
    pts, wid = lax.axis_size("pts"), lax.axis_size("wid")
    width = x.shape[1]
    head, slices = partition.shape
    heads = entry.shape[1] * wid // head
    mine = heads // wid
    rows = x.shape[0] // wid
    chunk = exit_m.shape[0]
    cells = heads * slices
    step = pick_tile(x.shape[0], (1024, 512, 256, 128))
    tile = pick_tile(rows, (1408, 256, 128))
    held = 256 // head
    share = 2
    for choice in (8, 4):
        if pts % choice == 0 and chunk % (16 * choice) == 0:
            share = choice
            break
    sizes = (pts, wid, share, step, tile, head, slices, heads)
    vmem = pl.BlockSpec(memory_space=pltpu.VMEM)
    hbm = pl.BlockSpec(memory_space=pltpu.HBM)
    dma = pltpu.SemaphoreType.DMA
    full = pltpu.VMEM((chunk * wid, width), BF16)
    hops = max(share // 2 - 1, 1)
    pin = lambda a: pltpu.with_memory_space_constraint(a, pltpu.HBM)
    weights, mix, own, upg, dng = pl.pallas_call(
        functools.partial(gather_kernel, sizes),
        name="slices_and_gather",
        out_shape=(
            pltpu.VMEM((rows, cells), BF16),
            pltpu.VMEM((cells, width), BF16),
            pltpu.VMEM((rows, width), BF16),
            full, full,
        ),
        in_specs=[hbm] * 8,
        out_specs=(vmem,) * 5,
        scratch_shapes=[
            pltpu.VMEM(x.shape, BF16),
            pltpu.VMEM((rows, width), BF16),
            pltpu.VMEM((wid,) + entry.shape, BF16),
            pltpu.VMEM((width, 256), BF16),
            pltpu.VMEM((2, step, 128), BF16),
            pltpu.VMEM((2, step, 256), F32),
            pltpu.VMEM((entry.shape[1] * wid, entry.shape[0]), BF16),
            pltpu.VMEM((chunk * wid, width), BF16),
            pltpu.VMEM((mine * slices + 16, 128), F32),
            pltpu.VMEM((held * slices + 16, held * head), F32),
            pltpu.VMEM((mine * slices, 128), F32),
            pltpu.VMEM((mine * slices, 128), F32),
            pltpu.VMEM((slices + 8, 128), F32),
            pltpu.VMEM((pts - 1, slices + 8, 128), F32),
            pltpu.VMEM(qkv.shape, F32),
            pltpu.VMEM((3, 128, 128), F32),
            pltpu.VMEM((wid, slices, 128), BF16),
            pltpu.VMEM((slices, head), BF16),
            pltpu.VMEM((1, head), F32),
            dma((x.shape[0] // step,)), dma((8,)),
            dma((4, wid - 1)), dma((4, wid - 1)),
            dma((4, wid - 1, hops)), dma((4, wid - 1, hops)),
            dma((4, wid - 1)), dma((4, wid - 1)),
            dma((pts - 1,)), dma((pts - 1,)),
            dma((wid - 1,)), dma((wid - 1,)),
        ],
        compiler_params=pltpu.CompilerParams(
            collective_id=0, has_side_effects=True, vmem_limit_bytes=44 * 1024 * 1024
        ),
    )(
        pin(x), pin(entry), pin(partition.T), pin(sharpness.reshape(1, head)), pin(qkv),
        pin(exit_m), pin(widening), pin(narrowing),
    )

    step = pick_tile(rows, (704, 256, 128))
    return pl.pallas_call(
        functools.partial(rows_kernel, step),
        name="mix_and_feed",
        out_shape=jax.ShapeDtypeStruct((rows, width), BF16),
        in_specs=[vmem] * 5,
        out_specs=pl.BlockSpec(memory_space=pl.ANY),
        scratch_shapes=[
            pltpu.VMEM((2, step, width), F32),
            pltpu.VMEM((2, step, width), BF16),
            pltpu.VMEM((rows // step, step, width), BF16),
            dma((rows // step,)),
        ],
        compiler_params=pltpu.CompilerParams(vmem_limit_bytes=40 * 1024 * 1024),
    )(weights, mix, own, upg, dng)


def solution(mesh):
    placed = (
        P("pts", None),
        P(None, "wid"),
        P(),
        P(),
        P(),
        P("wid", None),
        P("wid", None),
        P("wid", None),
    )
    return jax.shard_map(
        local, mesh=mesh, in_specs=placed, out_specs=P(("pts", "wid"), None), check_vma=False
    )
```

```python
import functools
import math

import jax
import jax.numpy as jnp
from jax import lax
from jax.experimental import pallas as pl
from jax.experimental.pallas import tpu as pltpu
from jax.sharding import PartitionSpec as P

MESH = pl.DeviceIdType.MESH
F32 = jnp.float32
BF16 = jnp.bfloat16
HIGH = lax.Precision.HIGHEST
LOG2E = math.log2(math.e)
BOTH = (((1,), (1,)), ((), ()))
GELU_A = math.sqrt(2.0 / math.pi)
GELU_B = 0.044715 * math.sqrt(2.0 / math.pi)


def layer_norm(values):
    centred = values - jnp.mean(values, axis=-1, keepdims=True)
    variance = jnp.mean(centred * centred, axis=-1, keepdims=True)
    return centred * lax.rsqrt(variance + 1e-05)


def pick_tile(rows, choices):
    for choice in choices:
        if rows % choice == 0:
            return choice
    return rows


def fold_rows(values, held, combine):
    shift = 4
    while shift >= held:
        values = combine(values, pltpu.roll(values, shift, 0))
        shift //= 2
    return values


def point_stats(stat, wide, model):
    mean = stat[wide + 16:wide + 24]
    shift = mean - mean.astype(BF16).astype(F32)
    variance = stat[wide + 24:wide + 32] * (1.0 / model) - shift * shift
    return mean, lax.rsqrt(variance + 1e-05)


def slice_softmax(stat, sums, mean, scale, held, slices):
    wide = held * slices
    points = stat.shape[1]
    across_points = lambda a: jnp.concatenate([a] * (points // 128), axis=1)
    raw = stat[wide:wide + 8] + stat[wide + 8:wide + 16]
    raw = (raw - mean * across_points(sums[wide:wide + 8] + sums[wide + 8:wide + 16])) * scale
    soft = jnp.maximum(raw, 0.0) + jnp.log1p(jnp.exp(-jnp.abs(raw)))
    inverse = LOG2E / (0.5 + soft) * scale
    shape = (wide // 8, 8, points)
    offset = across_points(sums[:wide]).reshape(shape) * mean[None]
    score = (stat[:wide].reshape(shape) - offset) * inverse[None]
    top = fold_rows(jnp.max(score, axis=0), held, jnp.maximum)
    power = jnp.exp2(score - top[None])
    return power, 1.0 / fold_rows(jnp.sum(power, axis=0), held, jnp.add)


def fill_logit_mat(mat, part_t, sharp, held, slices, head):
    wide = held * slices
    sharp_hi = sharp.astype(BF16).astype(F32)
    sharp_lo = sharp - sharp_hi
    small = lax.broadcasted_iota(jnp.int32, (8, head), 0) % held
    part = jnp.concatenate([part_t.astype(F32)] * (128 // head), axis=1)
    lane = lax.broadcasted_iota(jnp.int32, part.shape, 1)
    for h in range(held):
        lanes = slice(h * head, (h + 1) * head)
        mat[pl.ds(h, slices, stride=held), :] = jnp.where(lane // head == h, part, 0.0)
        mat[wide:wide + 8, lanes] = jnp.where(small == h, sharp_hi, 0.0)
        mat[wide + 8:wide + 16, lanes] = jnp.where(small == h, sharp_lo, 0.0)


def gather_kernel(
    sizes, x_ref, ent_ref, part_hbm, sharp_hbm, qkv_hbm, ex_ref, up_ref, dn_ref,
    w_ref, mix_ref, xo_ref, upg_ref, dng_ref,
    x_all, ent_buf, ep_buf, ext_buf, feats_buf, raw_buf, stat_buf, sums_buf, mean_all, scale_all,
    lhs_buf, lhs_sums, exg_ref, local_mat, num_buf, mass_buf,
    piece_out, piece_in, qkv_ref, big_qkv, tok_buf, part_ref, sharp_ref,
    x_sem, own_sem, zs_sem, zr_sem, fs_sem, fr_sem, cs_sem, cr_sem,
    a_send, a_recv, t_send, t_recv,
):
    pts, wid, share, step, tile, head, slices, heads = sizes
    p, w = lax.axis_index("pts"), lax.axis_index("wid")
    total_rows, model = x_all.shape
    rows = xo_ref.shape[0]
    steps = total_rows // step
    tiles = rows // tile
    chips = share // 2
    group, core = p // share, p % 2
    chip = (p % share) // 2
    member = core * chips + chip
    mine_heads = heads // wid
    local_lanes = mine_heads * head
    local_wide = mine_heads * slices
    fold = local_wide + 16
    chunk = ex_ref.shape[0]

    def x_copy(t):
        at = pl.ds(pl.multiple_of(t * step, step), step)
        return pltpu.make_async_copy(x_ref.at[at], x_all.at[at], x_sem.at[t])

    small_copies = [
        pltpu.make_async_copy(ent_ref, ent_buf, own_sem.at[0]),
        pltpu.make_async_copy(part_hbm, part_ref, own_sem.at[1]),
        pltpu.make_async_copy(sharp_hbm, sharp_ref, own_sem.at[2]),
        pltpu.make_async_copy(qkv_hbm, qkv_ref, own_sem.at[3]),
    ]
    for copy in small_copies[:1]:
        copy.start()
    for copy in small_copies[1:3]:
        copy.start()
    for t in range(min(2, steps)):
        x_copy(t).start()
    own_copies = []
    for m in range(1, 4):
        full = (exg_ref, upg_ref, dng_ref)[m - 1]
        own_copies.append(pltpu.make_async_copy(
            (ex_ref, up_ref, dn_ref)[m - 1],
            full.at[pl.ds(pl.multiple_of(w * chunk, chunk), chunk)], own_sem.at[m + 3],
        ))
    own_rows = pltpu.make_async_copy(
        x_ref.at[pl.ds(pl.multiple_of(w * rows, rows), rows)], xo_ref, own_sem.at[7]
    )

    barrier = pltpu.get_barrier_semaphore()
    for d in range(1, wid):
        pl.semaphore_signal(
            barrier, inc=1, device_id=(p, lax.rem(w + d, wid)), device_id_type=MESH
        )
    for d in range(1, pts):
        pl.semaphore_signal(
            barrier, inc=1, device_id=(lax.rem(p + d, pts), w), device_id_type=MESH
        )

    out_part = chunk // share
    paired = {2: 1, 3: 2} if chips == 4 else {}
    blocks_each = ep_buf.shape[1] // chips

    def spot(m, owner, whole=False):
        if m == 0:
            at = pl.ds(pl.multiple_of(core * (fold // 2), 8), fold // 2)
            if whole:
                return ep_buf.at[owner, :, at]
            return ep_buf.at[owner, pl.ds(chip * blocks_each, blocks_each), at]
        full = (exg_ref, upg_ref, dng_ref)[m - 1]
        if whole:
            part, count = core, chunk // 2
        elif m in paired:
            part, count = core * 2 + chip // paired[m] % 2, chunk // 4
        else:
            part, count = member, out_part
        return full.at[pl.ds(pl.multiple_of(owner * chunk + part * count, count), count)]

    def hops(m):
        return 1 if m in paired else chips - 1

    def across(m, d):
        return pltpu.make_async_remote_copy(
            src_ref=spot(m, w), dst_ref=spot(m, w),
            send_sem=zs_sem.at[m, d - 1], recv_sem=zr_sem.at[m, d - 1],
            device_id=(p, lax.rem(w + d, wid)), device_id_type=MESH,
        )

    def forward(m, d, e):
        owner = lax.rem(w - d + wid, wid)
        if m in paired:
            other = chip + paired[m] * (1 - 2 * (chip // paired[m] % 2))
        else:
            other = lax.rem(chip + e, chips)
        to = group * share + 2 * other + core
        return pltpu.make_async_remote_copy(
            src_ref=spot(m, owner), dst_ref=spot(m, owner),
            send_sem=fs_sem.at[m, d - 1, e - 1], recv_sem=fr_sem.at[m, d - 1, e - 1],
            device_id=(to, w), device_id_type=MESH,
        )

    def swap(m, d):
        owner = lax.rem(w - d + wid, wid)
        half = spot(m, owner, True)
        return pltpu.make_async_remote_copy(
            src_ref=half, dst_ref=half,
            send_sem=cs_sem.at[m, d - 1], recv_sem=cr_sem.at[m, d - 1],
            device_id=(p + 1 - 2 * core, w), device_id_type=MESH,
        )

    def cross_all():
        for m in range(4):
            for d in range(1, wid):
                across(m, d).start()

    def pass_on(m):
        for d in range(1, wid):
            across(m, d).wait_recv()
            for e in range(1, hops(m) + 1):
                forward(m, d, e).start()

    def trade(m):
        for d in range(1, wid):
            for e in range(1, hops(m) + 1):
                forward(m, d, e).wait_recv()
            swap(m, d).start()

    def traded(m):
        for d in range(1, wid):
            swap(m, d).wait_recv()

    with jax.named_scope("setup"):
        ext_buf[:, :128] = jnp.zeros((model, 128), BF16)
        piece_out[...] = jnp.zeros_like(piece_out)
        num_buf[...] = jnp.zeros_like(num_buf)
        mass_buf[...] = jnp.zeros_like(mass_buf)
        local_mat[...] = jnp.zeros_like(local_mat)
        for copy in small_copies[1:3]:
            copy.wait()
        for t in range(2, min(4, steps)):
            x_copy(t).start()
        for copy in own_copies:
            copy.start()
        fill_logit_mat(local_mat, part_ref[...], sharp_ref[...], mine_heads, slices, head)
        small_copies[0].wait()
        ext_buf[:, :local_lanes] = ent_buf[...]
        own = ext_buf[:, :128]
        column_sum = jnp.sum(own.astype(F32), axis=0, keepdims=True)
        main, fine = local_mat[...], local_mat[local_wide + 8:local_wide + 16]
        coarse = main[local_wide:local_wide + 8]
        blank = jnp.zeros((128 - local_wide - 16, 128), F32)
        first = jnp.concatenate([main[:local_wide], coarse, coarse, blank], axis=0)
        second = jnp.concatenate([jnp.zeros((local_wide, 128), F32), fine, fine, blank], axis=0)
        first, second = first.astype(BF16), second.astype(BF16)
        folded = lax.dot_general(own, first, BOTH, preferred_element_type=F32) + lax.dot_general(
            own, second, BOTH, preferred_element_type=F32
        )
        lanes = lax.broadcasted_iota(jnp.int32, folded.shape, 1)
        rounded = folded.astype(BF16).astype(F32)
        picked = jnp.where(
            jnp.logical_and(lanes >= local_wide + 8, lanes < local_wide + 16),
            folded - rounded, rounded,
        )
        picked = jnp.where(lanes >= local_wide + 16, 1.0 / model, picked)
        ext_buf[:, 128:] = picked.astype(BF16)

    def tile_at(t):
        return pl.ds(pl.multiple_of(t * step, step), step)

    def project(t):
        return jnp.dot(x_all[tile_at(t), :], ext_buf[...], preferred_element_type=F32)

    stat_lane = lax.broadcasted_iota(jnp.int32, (step, 128), 1)

    def prepare(t, slot):
        narrow = x_all[tile_at(t), :]
        rest = raw_buf[slot, :, 128:]
        mean = jnp.broadcast_to(rest[:, local_wide + 16:local_wide + 17], rest.shape)
        near = mean.astype(BF16)
        centred = narrow - jnp.concatenate([near] * (model // 128), axis=1)
        square = centred * centred
        while square.shape[1] > 128:
            half = square.shape[1] // 2
            square = square[:, :half] + square[:, half:]
        second = jnp.sum(square.astype(F32), axis=1, keepdims=True)
        feats_buf[slot] = (raw_buf[slot, :, :128] - mean * column_sum).astype(BF16)
        rest = jnp.where(stat_lane >= local_wide + 24, second, rest)
        stat_buf[slot] = rest.T[:local_wide + 32]

    def collect(t, slot):
        stat = stat_buf[slot]
        mean, scale = point_stats(stat, local_wide, model)
        mean_all[:, t * step:(t + 1) * step] = mean
        scale_all[:, t * step:(t + 1) * step] = scale
        power, total = slice_softmax(stat, sums_buf[...], mean, scale, mine_heads, slices)
        weights = (power * total[None]).reshape(local_wide, step)
        scaled = (power * (total * scale)[None]).reshape(local_wide, step).astype(BF16)
        num_buf[...] += jnp.dot(scaled, feats_buf[slot], preferred_element_type=F32)
        mass = weights[:, :128]
        for c in range(1, step // 128):
            mass = mass + weights[:, c * 128:(c + 1) * 128]
        mass_buf[...] += mass

    blocks = (steps + 1) // 2 + 2
    for b in range(blocks):
        if b == 1:
            with jax.named_scope("barrier"):
                pl.semaphore_wait(barrier, wid - 1 + pts - 1)
                for copy in own_copies:
                    copy.wait()
                cross_all()
                own_rows.start()
                small_copies[3].start()
        if b == blocks - 4:
            with jax.named_scope("pass0"):
                pass_on(0)
        with jax.named_scope("xwait"):
            for t in range(2 * b, min(2 * b + 2, steps)):
                x_copy(t).wait()
            for t in range(2 * b + 4, min(2 * b + 6, steps)):
                x_copy(t).start()
        with jax.named_scope("block"):
            for t in range(2 * b, min(2 * b + 2, steps)):
                raw_buf[t % 4] = project(t)
            if b == 0:
                folded = lax.dot_general(
                    first, own, BOTH, preferred_element_type=F32
                ) + lax.dot_general(second, own, BOTH, preferred_element_type=F32)
                row = lax.broadcasted_iota(jnp.int32, folded.shape, 0)
                rounded = folded.astype(BF16).astype(F32)
                picked = jnp.where(row >= local_wide + 8, folded - rounded, rounded)[:fold]
                for c in range(model // 128):
                    ep_buf[w, c] = picked[:, c * 128:(c + 1) * 128].astype(BF16)
                sums_buf[...] = lax.dot_general(
                    ext_buf[:, 128:], jnp.ones((model, 128), BF16), (((0,), (0,)), ((), ())),
                    preferred_element_type=F32,
                )
            for t in range(2 * b - 2, min(2 * b, steps)):
                if t >= 0:
                    prepare(t, t % 4)
            for t in range(2 * b - 4, min(2 * b - 2, steps)):
                if t >= 0:
                    collect(t, t % 4)
    with jax.named_scope("pack"):
        lane = lax.broadcasted_iota(jnp.int32, (slices, 128), 1)
        packed = jnp.zeros((slices, 128), F32)
        for h in range(mine_heads):
            packed = jnp.where(lane // head == h, num_buf[pl.ds(h, slices, stride=mine_heads), :], packed)
        masses = lax.dot_general(
            jnp.ones((8, 128), F32), mass_buf[...], BOTH, precision=HIGH,
            preferred_element_type=F32,
        )
        rounded = masses.astype(BF16).astype(F32)
        piece_out[:slices, :] = packed.astype(BF16)
        piece_out[slices:, :local_wide] = jnp.concatenate(
            [rounded, masses - rounded], axis=0
        ).astype(BF16)
        spread = []
        for d in range(1, pts):
            spread.append(pltpu.make_async_remote_copy(
                src_ref=piece_out, dst_ref=piece_in.at[d - 1],
                send_sem=a_send.at[d - 1], recv_sem=a_recv.at[d - 1],
                device_id=(lax.rem(p + d, pts), w), device_id_type=MESH,
            ))
        for copy in spread:
            copy.start()
    with jax.named_scope("pass1"):
        pass_on(1)
    with jax.named_scope("fill"):
        big_qkv[...] = jnp.zeros_like(big_qkv)
        small_copies[3].wait()
        for i in range(3):
            for h in range(mine_heads):
                at = slice(h * head, (h + 1) * head)
                big_qkv[i, at, at] = qkv_ref[i]
    with jax.named_scope("pass2"):
        pass_on(2)
    with jax.named_scope("pass3"):
        pass_on(3)
    with jax.named_scope("trade0"):
        trade(0)

    def slice_step(t, carry):
        at = pl.ds(pl.multiple_of(t * tile, tile), tile)
        there = pl.ds(pl.multiple_of(w * rows + t * tile, 128), tile)
        stat = lax.dot_general(lhs_buf[...], xo_ref[at, :], BOTH, preferred_element_type=F32)
        mean, scale = mean_all[:, there], scale_all[:, there]
        parts = []
        for owner in range(wid):
            mine = slice(owner * fold, (owner + 1) * fold)
            power, total = slice_softmax(
                stat[mine], lhs_sums[mine], mean, scale, mine_heads, slices
            )
            parts.append((power * total[None]).reshape(local_wide, tile).astype(BF16))
        w_ref[at, :] = jnp.concatenate(parts, axis=0).T
        return carry

    with jax.named_scope("sumwait"):
        total = piece_out[...].astype(F32)
        for d in range(1, pts):
            spread[d - 1].wait_recv()
            total = total + piece_in[d - 1].astype(F32)
        mass_row = total[slices:slices + 1] + total[slices + 8:slices + 9]
    with jax.named_scope("token"):
        row = lax.broadcasted_iota(jnp.int32, (slices, local_wide), 0)
        col = lax.broadcasted_iota(jnp.int32, (slices, local_wide), 1)
        masses = jnp.ones((slices, 128), F32)
        for h in range(mine_heads):
            one = jnp.sum(
                jnp.where(col == row * mine_heads + h, mass_row[:, :local_wide], 0.0),
                axis=1, keepdims=True,
            )
            masses = jnp.where(lane // head == h, one, masses)
        tokens = total[:slices] / (masses + 1e-05)
        queries, keys_all, value_rows = (
            jnp.dot(tokens, big_qkv[i], precision=HIGH, preferred_element_type=F32) for i in range(3)
        )
        stacked = lambda a: jnp.concatenate(
            [jnp.where(lane // head == h, a, 0.0) for h in range(mine_heads)], axis=0
        )
        scores = lax.dot_general(
            queries, stacked(keys_all), BOTH, precision=HIGH, preferred_element_type=F32
        ) * (1.0 / head ** 0.5)
        owner_head = col // slices
        attend = jnp.zeros_like(scores)
        for h in range(mine_heads):
            part = jnp.where(owner_head == h, scores, -jnp.inf)
            power = jnp.exp(part - jnp.max(part, axis=1, keepdims=True))
            attend = attend + power / jnp.sum(power, axis=1, keepdims=True)
        tok_buf[w] = jnp.dot(
            attend, stacked(value_rows), precision=HIGH, preferred_element_type=F32
        ).astype(BF16)
        ring = []
        for d in range(1, wid):
            ring.append(pltpu.make_async_remote_copy(
                src_ref=tok_buf.at[w], dst_ref=tok_buf.at[w],
                send_sem=t_send.at[d - 1], recv_sem=t_recv.at[d - 1],
                device_id=(p, lax.rem(w + d, wid)), device_id_type=MESH,
            ))
        for copy in ring:
            copy.start()
    with jax.named_scope("traded0"):
        traded(0)
        own_rows.wait()
    with jax.named_scope("entt"):
        for owner in range(wid):
            for c in range(model // 128):
                lhs_buf[owner * fold:(owner + 1) * fold, c * 128:(c + 1) * 128] = ep_buf[owner, c]
        lhs_sums[...] = jnp.dot(
            lhs_buf[...], jnp.ones((model, 128), BF16), preferred_element_type=F32
        )
    with jax.named_scope("slice"):
        lax.fori_loop(0, tiles // 2, slice_step, 0)
    with jax.named_scope("trade1"):
        trade(1)
    with jax.named_scope("slice"):
        lax.fori_loop(tiles // 2, tiles, slice_step, 0)
    with jax.named_scope("ringwait"):
        for m in range(2, 4):
            trade(m)
        traded(1)
        for copy in ring:
            copy.wait_recv()
    with jax.named_scope("mix"):
        row = lax.broadcasted_iota(jnp.int32, (local_wide, slices), 0) // mine_heads
        col = lax.broadcasted_iota(jnp.int32, (local_wide, slices), 1)
        repeat = jnp.where(row == col, 1.0, 0.0).astype(BF16)
        row = lax.broadcasted_iota(jnp.int32, (local_wide, 128), 0) % mine_heads
        col = lax.broadcasted_iota(jnp.int32, (local_wide, 128), 1) // head
        for z in range(wid):
            block = jnp.dot(repeat, tok_buf[z], preferred_element_type=F32)
            block = jnp.where(row == col, block, 0.0).astype(BF16)[:, :local_lanes]
            mix_ref[z * local_wide:(z + 1) * local_wide, :] = jnp.dot(
                block, exg_ref[z * local_lanes:(z + 1) * local_lanes, :],
                preferred_element_type=F32,
            ).astype(BF16)
    with jax.named_scope("drain"):
        for m in range(2, 4):
            traded(m)
        for m in range(4):
            for d in range(1, wid):
                across(m, d).wait_send()
                swap(m, d).wait_send()
                for e in range(1, hops(m) + 1):
                    forward(m, d, e).wait_send()
        for copy in spread + ring:
            copy.wait_send()


def rows_kernel(
    step, w_ref, mix_ref, x_ref, upg_ref, dng_ref, out_ref,
    mid_buf, normed_buf, out_buf, out_sem,
):
    steps = x_ref.shape[0] // step
    model = x_ref.shape[1]

    def tile_at(t):
        return pl.ds(pl.multiple_of(t * step, step), step)

    def out_copy(t):
        return pltpu.make_async_copy(out_buf.at[t], out_ref.at[tile_at(t)], out_sem.at[t])

    def mix(t, slot):
        at = tile_at(t)
        midway = x_ref[at, :].astype(F32) + jnp.dot(
            w_ref[at, :], mix_ref[...], preferred_element_type=F32
        )
        mid_buf[slot] = midway
        centred = (midway - jnp.mean(midway, axis=1, keepdims=True)).astype(BF16)
        square = centred * centred
        while square.shape[1] > 128:
            half = square.shape[1] // 2
            square = square[:, :half] + square[:, half:]
        variance = jnp.sum(square.astype(F32), axis=1, keepdims=True) * (1.0 / model)
        scale = lax.rsqrt(variance + 1e-05).astype(BF16)
        normed_buf[slot] = centred * scale

    def feed(t, slot):
        before = jnp.dot(
            normed_buf[slot], upg_ref[...], preferred_element_type=F32
        ).astype(BF16)
        inner = before * (GELU_A + GELU_B * (before * before))
        half = 0.5 * before
        hidden = half + half * jnp.tanh(inner)
        out_buf[t] = (
            mid_buf[slot] + jnp.dot(hidden, dng_ref[...], preferred_element_type=F32)
        ).astype(BF16)

    with jax.named_scope("first"):
        mix(0, 0)
    for t in range(steps):
        with jax.named_scope("tail"):
            slot = t % 2
            if t + 1 < steps:
                mix(t + 1, 1 - slot)
            feed(t, slot)
            out_copy(t).start()
    with jax.named_scope("outwait"):
        for t in range(steps):
            out_copy(t).wait()


def local(x, entry, partition, sharpness, qkv, exit_m, widening, narrowing):
    pts, wid = lax.axis_size("pts"), lax.axis_size("wid")
    width = x.shape[1]
    head, slices = partition.shape
    heads = entry.shape[1] * wid // head
    mine = heads // wid
    rows = x.shape[0] // wid
    chunk = exit_m.shape[0]
    cells = heads * slices
    step = pick_tile(x.shape[0], (1024, 512, 256, 128))
    tile = pick_tile(rows, (1408, 256, 128))
    fold = mine * slices + 16
    share = 2
    for choice in (8, 4):
        if pts % choice == 0 and chunk % (16 * choice) == 0:
            share = choice
            break
    sizes = (pts, wid, share, step, tile, head, slices, heads)
    vmem = pl.BlockSpec(memory_space=pltpu.VMEM)
    hbm = pl.BlockSpec(memory_space=pltpu.HBM)
    dma = pltpu.SemaphoreType.DMA
    full = pltpu.VMEM((chunk * wid, width), BF16)
    hops = max(share // 2 - 1, 1)
    pin = lambda a: pltpu.with_memory_space_constraint(a, pltpu.HBM)
    weights, mix, own, upg, dng = pl.pallas_call(
        functools.partial(gather_kernel, sizes),
        name="slices_and_gather",
        out_shape=(
            pltpu.VMEM((rows, cells), BF16),
            pltpu.VMEM((cells, width), BF16),
            pltpu.VMEM((rows, width), BF16),
            full, full,
        ),
        in_specs=[hbm] * 8,
        out_specs=(vmem,) * 5,
        scratch_shapes=[
            pltpu.VMEM(x.shape, BF16),
            pltpu.VMEM(entry.shape, BF16),
            pltpu.VMEM((wid, width // 128, fold, 128), BF16),
            pltpu.VMEM((width, 256), BF16),
            pltpu.VMEM((4, step, 128), BF16),
            pltpu.VMEM((4, step, 256), F32),
            pltpu.VMEM((4, mine * slices + 32, step), F32),
            pltpu.VMEM((128, 128), F32),
            pltpu.VMEM((8, x.shape[0]), F32),
            pltpu.VMEM((8, x.shape[0]), F32),
            pltpu.VMEM((wid * fold, width), BF16),
            pltpu.VMEM((wid * fold, 128), F32),
            pltpu.VMEM((chunk * wid, width), BF16),
            pltpu.VMEM((fold, 128), F32),
            pltpu.VMEM((mine * slices, 128), F32),
            pltpu.VMEM((mine * slices, 128), F32),
            pltpu.VMEM((slices + 16, 128), BF16),
            pltpu.VMEM((pts - 1, slices + 16, 128), BF16),
            pltpu.VMEM(qkv.shape, F32),
            pltpu.VMEM((3, 128, 128), F32),
            pltpu.VMEM((wid, slices, 128), BF16),
            pltpu.VMEM((slices, head), BF16),
            pltpu.VMEM((1, head), F32),
            dma((x.shape[0] // step,)), dma((8,)),
            dma((4, wid - 1)), dma((4, wid - 1)),
            dma((4, wid - 1, hops)), dma((4, wid - 1, hops)),
            dma((4, wid - 1)), dma((4, wid - 1)),
            dma((pts - 1,)), dma((pts - 1,)),
            dma((wid - 1,)), dma((wid - 1,)),
        ],
        compiler_params=pltpu.CompilerParams(
            collective_id=0, has_side_effects=True, vmem_limit_bytes=44 * 1024 * 1024
        ),
    )(
        pin(x), pin(entry), pin(partition.T), pin(sharpness.reshape(1, head)), pin(qkv),
        pin(exit_m), pin(widening), pin(narrowing),
    )

    step = pick_tile(rows, (704, 256, 128))
    return pl.pallas_call(
        functools.partial(rows_kernel, step),
        name="mix_and_feed",
        out_shape=jax.ShapeDtypeStruct((rows, width), BF16),
        in_specs=[vmem] * 5,
        out_specs=pl.BlockSpec(memory_space=pl.ANY),
        scratch_shapes=[
            pltpu.VMEM((2, step, width), F32),
            pltpu.VMEM((2, step, width), BF16),
            pltpu.VMEM((rows // step, step, width), BF16),
            dma((rows // step,)),
        ],
        compiler_params=pltpu.CompilerParams(vmem_limit_bytes=40 * 1024 * 1024),
    )(weights, mix, own, upg, dng)


def solution(mesh):
    placed = (
        P("pts", None),
        P(None, "wid"),
        P(),
        P(),
        P(),
        P("wid", None),
        P("wid", None),
        P("wid", None),
    )
    return jax.shard_map(
        local, mesh=mesh, in_specs=placed, out_specs=P(("pts", "wid"), None), check_vma=False
    )
```
